128 devices in a mesh: row: 64 (over z, y, x), col: 2 (over core).
Axes of the slice: x: 4, y: 4, z: 4, core: 2. Of those that a mesh axis runs over, the one named last changes fastest.
Arguments:
- matrix: float32 [12288, 12288], P('row', 'col'), may hold values from -2 to 2, as said below
- diagonal: float32 [12288], P(('row', 'col')), may hold values from 1 to 6
- start: float32 [12288], P(('row', 'col')), may hold values from -6 to 6
Outputs:
- basis: float32 [4, 12288], P(None, ('row', 'col'))
- coefficients: float32 [2, 3], replicated
The draws below stay inside these ranges and needn't reach their ends.
Inputs may be any that keep to these rules, and one draw needn't show every extreme that they name: matrix is exactly symmetric, its entries of order one over the square root of 12288.
All inputs are finite; a program needn't handle non-finite values.
Results may differ from the reference program's by a relative error of at most 0.0003.
Values sent between devices are 32-bit elements.
A program may use at most 64 MiB of HBM per device.

```python
import math
import jax
import jax.numpy as jnp
from jax import lax

ITERS = 3
DIM = 12288


def draw_matrix(key, part):
    raw_draw = jax.random.normal(key, (DIM, DIM), jnp.float32)
    return (raw_draw + raw_draw.T) * (1.0 / math.sqrt(2.0 * DIM))


def steps_of(key, extent, cuts, low, high):
    def one(position, shards_of):
        heights = jax.random.uniform(jax.random.fold_in(jax.random.fold_in(key, 6), position), (shards_of,), jnp.float32, low / len(cuts), high / len(cuts))
        return jnp.repeat(jnp.exp(heights), extent[position] // shards_of).reshape((-1,) + (1,) * (len(extent) - position - 1))

    level = one(*cuts[0])
    for cut in cuts[1:]:
        level = level * one(*cut)
    return level


def bell_draw(rng, dims, scale, most, cuts=(), dtype=jnp.bfloat16):
    array = scale * jax.random.normal(rng, dims, jnp.float32)
    if cuts:
        array = array * steps_of(rng, dims, cuts, -0.22, 0.18)
    return jnp.clip(array, -most, most).astype(dtype)


def setup_inputs(seed: int = 0) -> dict:
    streams_of = jax.random.split(jax.random.key(seed), 4)
    return {
        "matrix": draw_matrix(jax.random.fold_in(streams_of[3], 71), 0),
        "diagonal": jnp.clip(jnp.exp(math.log(6.0) - 1.7917595 * jax.random.uniform(streams_of[1], (DIM,), jnp.float32) ** steps_of(streams_of[1], (DIM,), ((0, 128),), -0.2, 0.2)), 1.0, 6.0),
        "start": bell_draw(streams_of[2], (DIM,), 1.0, 6.0, ((0, 128),), jnp.float32),
    }


def reference(matrix, diagonal, start):
    full_dim = start.shape[0]
    current = start / jnp.sqrt(jnp.sum(start * start))
    basis_rows = jnp.zeros((ITERS + 1, full_dim), jnp.float32).at[0].set(current)
    alpha_list = []
    beta_list = []
    for iteration in range(ITERS):
        image = jnp.dot(matrix, current, precision=lax.Precision.HIGHEST, preferred_element_type=jnp.float32) + diagonal * current
        intersect = jnp.dot(basis_rows, image, precision=lax.Precision.HIGHEST, preferred_element_type=jnp.float32)
        image = image - jnp.dot(intersect, basis_rows, precision=lax.Precision.HIGHEST, preferred_element_type=jnp.float32)
        beta_value = jnp.sqrt(jnp.sum(image * image))
        current = image / beta_value
        basis_rows = basis_rows.at[iteration + 1].set(current)
        alpha_list.append(intersect[iteration])
        beta_list.append(beta_value)
    coefficients = jnp.stack([jnp.stack(alpha_list), jnp.stack(beta_list)])
    return (basis_rows * jnp.sqrt(jnp.float32(full_dim)), coefficients)
```

```python
import math

import jax
import jax.numpy as jnp
from jax import lax
from jax.experimental import pallas as pl
from jax.experimental.pallas import tpu as pltpu
from jax.sharding import PartitionSpec as P

ITERS = 3
DIM = 12288
DEVICES = 128
ROWS = 192
COLS = 6144
TILE = 96
LANES = 128
PAIRS = 32
LOGICAL = pl.DeviceIdType.LOGICAL


def hops(step):
    return (0, 1, 2, 1)[step]


STEPS = sorted(
    (
        (i, j, k, m)
        for i in range(4)
        for j in range(4)
        for k in range(4)
        for m in range(2)
        if i or j or k or m
    ),
    key=lambda s: (-(hops(s[0]) + hops(s[1]) + hops(s[2])), s[3]),
)


def total(value):
    return jnp.sum(value, keepdims=True)


def kernel(matrix, diagonal, start, basis, coef, mat, frame, slots, x_rows, mat_sem, send_sem, recv_sem):
    row = lax.axis_index("row")
    col = lax.axis_index("col")
    me = row * 2 + col
    pair = row // 2
    odd = row % 2
    z, y, x = row // 16, (row // 4) % 4, row % 4
    z_part = [((z + i) % 4) * 32 for i in range(4)]
    y_part = [((y + i) % 4) * 8 for i in range(4)]
    x_part = [((x + i) % 4) * 2 for i in range(4)]
    c_part = [col, 1 - col]
    peers = [z_part[i] + y_part[j] + x_part[k] + c_part[m] for i, j, k, m in STEPS]

    barrier = pltpu.get_barrier_semaphore()
    for peer in peers:
        pl.semaphore_signal(barrier, inc=1, device_id=peer, device_id_type=LOGICAL)
    load = pltpu.make_async_copy(matrix, mat, mat_sem)
    load.start()

    lane = lax.broadcasted_iota(jnp.int32, (1, LANES), 1)

    def framed(part):
        wide = jnp.concatenate([part, jnp.zeros((1, LANES - TILE), jnp.float32)], axis=1)
        out = []
        for o in range(2):
            for c in range(2):
                offset = 64 * o + TILE * c
                shift = offset % LANES
                moved = pltpu.roll(wide, shift, 1) if shift else wide
                first, second = jnp.where(lane >= shift, moved, 0.0), jnp.where(lane < shift, moved, 0.0)
                zero = jnp.zeros_like(moved)
                out.append((zero, first) if offset >= LANES else (first, second))
        here = odd * 2 + col
        rows = []
        for h in range(2):
            pick = out[0][h]
            for n in range(1, 4):
                pick = jnp.where(here == n, out[n][h], pick)
            rows.append(pick)
        return jnp.concatenate(rows, axis=0)

    diag_frame = framed(diagonal[...])
    first_frame = framed(start[...])

    def exchange(k, value):
        frame[k] = value
        slots[k, me] = value
        for peer in peers:
            pltpu.make_async_remote_copy(
                src_ref=frame.at[k],
                dst_ref=slots.at[k, me],
                send_sem=send_sem.at[k],
                recv_sem=recv_sem.at[k],
                device_id=peer,
                device_id_type=LOGICAL,
            ).start()
        arrived = slots.at[k, 0 : DEVICES - 1]
        pltpu.make_async_copy(arrived, arrived, recv_sem.at[k]).wait()
        both = slots[k].reshape(PAIRS, 2, 2, 2, LANES)
        both = both[:, :, 0] + both[:, :, 1]
        even, uneven = both[:, 0], both[:, 1]
        return jnp.concatenate([even[:, 0:1], even[:, 1:2] + uneven[:, 0:1], uneven[:, 1:2]], axis=1)

    def rows_of(vector):
        return vector.reshape(3 * PAIRS, LANES)

    def multiply(vector):
        x_rows[...] = vector
        half = col * (3 * PAIRS // 2)

        def step(n, acc):
            value = x_rows[pl.ds(half + n, 1), :]
            wide = jnp.broadcast_to(value, (8, LANES))
            at = pl.multiple_of(n * LANES, LANES)
            return tuple(
                a + mat[8 * g : 8 * g + 8, pl.ds(at, LANES)] * wide for g, a in enumerate(acc)
            )

        acc = tuple(jnp.zeros((8, LANES), jnp.float32) for _ in range(ROWS // 8))
        acc = lax.fori_loop(0, COLS // LANES, step, acc, unroll=4)
        zero = jnp.zeros((8, LANES), jnp.float32)
        is_odd = odd == 1
        padded = [
            jnp.where(is_odd, acc[t - 8] if t >= 8 else zero, acc[t] if t < 24 else zero) for t in range(32)
        ]
        out = []
        for h in range(2):
            block = jnp.concatenate(padded[16 * h : 16 * h + 16], axis=0)
            out.append(jnp.sum(block.T, axis=0, keepdims=True))
        own = x_rows[pl.ds(pair * 3 + odd, 2), :]
        return jnp.concatenate(out, axis=0) + diag_frame * own

    def unframed(vector):
        x_rows[...] = vector
        own = x_rows[pl.ds(pair * 3 + odd, 2), :]
        first, second = own[0:1], own[1:2]
        pick = None
        for o in range(2):
            for c in range(2):
                offset = 64 * o + TILE * c
                shift = offset % LANES
                if offset >= LANES:
                    moved = pltpu.roll(second, LANES - shift, 1)
                elif shift:
                    moved = pltpu.roll(jnp.where(lane >= shift, first, second), LANES - shift, 1)
                else:
                    moved = first
                pick = moved if pick is None else jnp.where(odd * 2 + col == 2 * o + c, moved, pick)
        return pick[:, :TILE]

    pl.semaphore_wait(barrier, DEVICES - 1)

    scale = jnp.float32(math.sqrt(DIM))
    vector = rows_of(exchange(0, first_frame))
    vector = vector / jnp.sqrt(total(vector * vector))
    basis[0:1, :] = unframed(vector) * scale
    load.wait()
    known = [vector]
    alpha, beta = [], []
    for k in range(ITERS):
        image = rows_of(exchange(k + 1, multiply(known[-1])))
        dots = [total(q * image) for q in known]
        for h, q in zip(dots, known):
            image = image - h * q
        norm = jnp.sqrt(total(image * image))
        vector = image / norm
        basis[k + 1 : k + 2, :] = unframed(vector) * scale
        known.append(vector)
        alpha.append(dots[-1])
        beta.append(norm)
    coef[...] = jnp.concatenate(
        [jnp.concatenate(alpha, axis=1), jnp.concatenate(beta, axis=1)], axis=0
    )
    for k in range(ITERS + 1):
        sent = slots.at[k, 0 : DEVICES - 1]
        pltpu.make_async_copy(sent, sent, send_sem.at[k]).wait()


def solution(mesh):
    def local(matrix, diagonal, start):
        return pl.pallas_call(
            kernel,
            out_shape=(
                jax.ShapeDtypeStruct((ITERS + 1, TILE), jnp.float32),
                jax.ShapeDtypeStruct((2, ITERS), jnp.float32),
            ),
            in_specs=[
                pl.BlockSpec(memory_space=pl.ANY),
                pl.BlockSpec(memory_space=pltpu.VMEM),
                pl.BlockSpec(memory_space=pltpu.VMEM),
            ],
            out_specs=(pl.BlockSpec(memory_space=pltpu.VMEM), pl.BlockSpec(memory_space=pltpu.VMEM)),
            scratch_shapes=[
                pltpu.VMEM((ROWS, COLS), jnp.float32),
                pltpu.VMEM((ITERS + 1, 2, LANES), jnp.float32),
                pltpu.VMEM((ITERS + 1, DEVICES, 2, LANES), jnp.float32),
                pltpu.VMEM((3 * PAIRS, LANES), jnp.float32),
                pltpu.SemaphoreType.DMA,
                pltpu.SemaphoreType.DMA((ITERS + 1,)),
                pltpu.SemaphoreType.DMA((ITERS + 1,)),
            ],
            compiler_params=pltpu.CompilerParams(collective_id=0, has_side_effects=True),
        )(matrix, diagonal.reshape(1, TILE), start.reshape(1, TILE))

    return jax.shard_map(
        local,
        mesh=mesh,
        in_specs=(P("row", "col"), P(("row", "col")), P(("row", "col"))),
        out_specs=(P(None, ("row", "col")), P()),
        check_vma=False,
    )
```

```python
import math

import jax
import jax.numpy as jnp
from jax import lax
from jax.experimental import pallas as pl
from jax.experimental.pallas import tpu as pltpu
from jax.sharding import PartitionSpec as P

ITERS = 3
DIM = 12288
DEVICES = 128
ROWS = 192
COLS = 6144
TILE = 96
LANES = 128
PAIRS = 32
LOGICAL = pl.DeviceIdType.LOGICAL


def hops(step):
    return (0, 1, 2, 1)[step]


STEPS = sorted(
    (
        (i, j, k, m)
        for i in range(4)
        for j in range(4)
        for k in range(4)
        for m in range(2)
        if i or j or k or m
    ),
    key=lambda s: (-(hops(s[0]) + hops(s[1]) + hops(s[2])), s[3]),
)


def total(value):
    return jnp.sum(value, keepdims=True)


def kernel(matrix, diagonal, start, out, mat, small, frame, planes, x_rows, slots, mat_sem, small_sem, send_sem, recv_sem):
    row = lax.axis_index("row")
    col = lax.axis_index("col")
    pair = row // 2
    odd = row % 2
    here = odd * 2 + col
    z, y, x = row // 16, (row // 4) % 4, row % 4
    z_part = [((z + i) % 4) * 32 for i in range(4)]
    y_part = [((y + i) % 4) * 8 for i in range(4)]
    x_part = [((x + i) % 4) * 2 for i in range(4)]
    c_part = [col, 1 - col]
    peers = [z_part[i] + y_part[j] + x_part[k] + c_part[m] for i, j, k, m in STEPS]

    barrier = pltpu.get_barrier_semaphore()
    for peer in peers:
        pl.semaphore_signal(barrier, inc=1, device_id=peer, device_id_type=LOGICAL)
    load_start = pltpu.make_async_copy(start, small.at[0], small_sem.at[0])
    load_diag = pltpu.make_async_copy(diagonal, small.at[1], small_sem.at[1])
    load = pltpu.make_async_copy(matrix, mat, mat_sem)
    load_start.start()
    load_diag.start()
    load.start()

    lane = lax.broadcasted_iota(jnp.int32, (1, LANES), 1)

    def framed(part):
        wide = jnp.concatenate([part, jnp.zeros((1, LANES - TILE), jnp.float32)], axis=1)
        out = []
        for o in range(2):
            for c in range(2):
                offset = 64 * o + TILE * c
                shift = offset % LANES
                moved = pltpu.roll(wide, shift, 1) if shift else wide
                first, second = jnp.where(lane >= shift, moved, 0.0), jnp.where(lane < shift, moved, 0.0)
                zero = jnp.zeros_like(moved)
                out.append((zero, first) if offset >= LANES else (first, second))
        rows = []
        for h in range(2):
            pick = out[0][h]
            for n in range(1, 4):
                pick = jnp.where(here == n, out[n][h], pick)
            rows.append(pick)
        return rows

    def send(k, value):
        for h in range(2):
            frame[k, h] = value[h]
        for peer in peers:
            pltpu.make_async_remote_copy(
                src_ref=frame.at[k],
                dst_ref=planes.at[k, here, :, pl.ds(pair, 1), :],
                send_sem=send_sem.at[k],
                recv_sem=recv_sem.at[k],
                device_id=peer,
                device_id_type=LOGICAL,
            ).start()
        for h in range(2):
            planes[k, here, h, pl.ds(pair, 1), :] = value[h]

    def counted(sem):
        done = slots.at[:]
        return pltpu.make_async_copy(done, done, sem)

    def receive(k):
        counted(recv_sem.at[k]).wait()
        part = [planes[k, 0, h] + planes[k, 1, h] for h in range(2)]
        rest = [planes[k, 2, h] + planes[k, 3, h] for h in range(2)]
        rows = [part[0], part[1] + rest[0], rest[1]]
        for j in range(3):
            x_rows[j] = rows[j]
        return jnp.concatenate(rows, axis=0)

    def own_rows():
        return [x_rows[odd + h, pl.ds(pair, 1), :] for h in range(2)]

    def multiply(diag):
        own = own_rows()
        acc = [None] * (ROWS // 8)
        for n in range(COLS // LANES):
            value = x_rows[n % 3, pl.ds(col * (PAIRS // 2) + n // 3, 1), :]
            wide = jnp.broadcast_to(value, (8, LANES))
            for g in range(ROWS // 8):
                term = mat[8 * g : 8 * g + 8, n * LANES : (n + 1) * LANES] * wide
                acc[g] = term if n == 0 else acc[g] + term
        zero = jnp.zeros((8, LANES), jnp.float32)
        is_odd = odd == 1
        padded = [
            jnp.where(is_odd, acc[t - 8] if t >= 8 else zero, acc[t] if t < 24 else zero) for t in range(32)
        ]
        rows = []
        for h in range(2):
            block = jnp.concatenate(padded[16 * h : 16 * h + 16], axis=0)
            rows.append(jnp.sum(block.T, axis=0, keepdims=True) + diag[h] * own[h])
        return rows

    def unframed(first, second):
        pick = None
        for o in range(2):
            for c in range(2):
                offset = 64 * o + TILE * c
                shift = offset % LANES
                if offset >= LANES:
                    moved = pltpu.roll(second, LANES - shift, 1)
                elif shift:
                    moved = pltpu.roll(jnp.where(lane >= shift, first, second), LANES - shift, 1)
                else:
                    moved = first
                pick = moved if pick is None else jnp.where(here == 2 * o + c, moved, pick)
        return pick

    load_start.wait()
    first = framed(small[0])
    load_diag.wait()
    diag = framed(small[1])
    pl.semaphore_wait(barrier, DEVICES - 1)
    send(0, first)
    load.wait()

    scale = jnp.float32(math.sqrt(DIM))
    known, images, slices = [], [], []
    for k in range(ITERS + 1):
        vector = receive(k)
        own = unframed(*own_rows())
        if k < ITERS:
            image = multiply(diag)
        dots = [total(q * vector) for q in known]
        for h, q, s in zip(dots, known, slices):
            vector = vector - h * q
            own = own - h * s
        norm = jnp.sqrt(total(vector * vector))
        if k < ITERS:
            for h, f in zip(dots, images):
                image = [a - h * b for a, b in zip(image, f)]
            image = [a / norm for a in image]
            send(k + 1, image)
            images.append(image)
            known.append(vector / norm)
        own = own / norm
        slices.append(own)
        out[k : k + 1, :] = own * scale
        if k:
            column = lane == k - 1
            a_row = jnp.where(column, dots[-1], a_row if k > 1 else 0.0)
            b_row = jnp.where(column, norm, b_row if k > 1 else 0.0)
    out[4:5, :] = a_row
    out[5:6, :] = b_row
    for k in range(ITERS + 1):
        counted(send_sem.at[k]).wait()


def split_kernel(packed, basis, coef):
    basis[...] = packed[0:4, 0:TILE]
    coef[...] = packed[4:6, 0:ITERS]


def solution(mesh):
    vmem = pl.BlockSpec(memory_space=pltpu.VMEM)
    hbm = pl.BlockSpec(memory_space=pl.ANY)

    def local(matrix, diagonal, start):
        packed = pl.pallas_call(
            kernel,
            out_shape=pltpu.VMEM((8, LANES), jnp.float32),
            in_specs=[hbm, hbm, hbm],
            out_specs=vmem,
            scratch_shapes=[
                pltpu.VMEM((ROWS, COLS), jnp.float32),
                pltpu.VMEM((2, 1, TILE), jnp.float32),
                pltpu.VMEM((ITERS + 1, 2, 1, LANES), jnp.float32),
                pltpu.VMEM((ITERS + 1, 4, 2, PAIRS, LANES), jnp.float32),
                pltpu.VMEM((3, PAIRS, LANES), jnp.float32),
                pltpu.VMEM((DEVICES - 1, 2, LANES), jnp.float32),
                pltpu.SemaphoreType.DMA,
                pltpu.SemaphoreType.DMA((2,)),
                pltpu.SemaphoreType.DMA((ITERS + 1,)),
                pltpu.SemaphoreType.DMA((ITERS + 1,)),
            ],
            compiler_params=pltpu.CompilerParams(collective_id=0, has_side_effects=True),
        )(matrix, diagonal.reshape(1, TILE), start.reshape(1, TILE))
        return pl.pallas_call(
            split_kernel,
            out_shape=(
                jax.ShapeDtypeStruct((ITERS + 1, TILE), jnp.float32),
                jax.ShapeDtypeStruct((2, ITERS), jnp.float32),
            ),
            in_specs=[vmem],
            out_specs=(vmem, vmem),
        )(packed)

    return jax.shard_map(
        local,
        mesh=mesh,
        in_specs=(P("row", "col"), P(("row", "col")), P(("row", "col"))),
        out_specs=(P(None, ("row", "col")), P()),
        check_vma=False,
    )
```

```python
import math

import jax
import jax.numpy as jnp
from jax import lax
from jax.experimental import pallas as pl
from jax.experimental.pallas import tpu as pltpu
from jax.sharding import PartitionSpec as P

ITERS = 3
DIM = 12288
DEVICES = 128
ROWS = 192
COLS = 6144
TILE = 96
LANES = 128
PAIRS = 32
LOGICAL = pl.DeviceIdType.LOGICAL


def hops(step):
    return (0, 1, 2, 1)[step]


STEPS = sorted(
    (
        (i, j, k, m)
        for i in range(4)
        for j in range(4)
        for k in range(4)
        for m in range(2)
        if i or j or k or m
    ),
    key=lambda s: (-(hops(s[0]) + hops(s[1]) + hops(s[2])), s[3]),
)


def total(value):
    return jnp.sum(value, keepdims=True)


def kernel(matrix, diagonal, start, out, mat, small, frame, planes, x_rows, slots, mat_sem, small_sem, send_sem, recv_sem):
    row = lax.axis_index("row")
    col = lax.axis_index("col")
    pair = row // 2
    odd = row % 2
    here = odd * 2 + col
    z, y, x = row // 16, (row // 4) % 4, row % 4
    z_part = [((z + i) % 4) * 32 for i in range(4)]
    y_part = [((y + i) % 4) * 8 for i in range(4)]
    x_part = [((x + i) % 4) * 2 for i in range(4)]
    c_part = [col, 1 - col]
    peers = [z_part[i] + y_part[j] + x_part[k] + c_part[m] for i, j, k, m in STEPS]

    barrier = pltpu.get_barrier_semaphore()
    for peer in peers:
        pl.semaphore_signal(barrier, inc=1, device_id=peer, device_id_type=LOGICAL)
    load_start = pltpu.make_async_copy(start, small.at[0], small_sem.at[0])
    load_diag = pltpu.make_async_copy(diagonal, small.at[1], small_sem.at[1])
    load = pltpu.make_async_copy(matrix, mat, mat_sem)
    load_start.start()
    load_diag.start()
    load.start()

    lane = lax.broadcasted_iota(jnp.int32, (1, LANES), 1)

    def framed(part):
        wide = jnp.concatenate([part, jnp.zeros((1, LANES - TILE), jnp.float32)], axis=1)
        out = []
        for o in range(2):
            for c in range(2):
                offset = 64 * o + TILE * c
                shift = offset % LANES
                moved = pltpu.roll(wide, shift, 1) if shift else wide
                first, second = jnp.where(lane >= shift, moved, 0.0), jnp.where(lane < shift, moved, 0.0)
                zero = jnp.zeros_like(moved)
                out.append((zero, first) if offset >= LANES else (first, second))
        rows = []
        for h in range(2):
            pick = out[0][h]
            for n in range(1, 4):
                pick = jnp.where(here == n, out[n][h], pick)
            rows.append(pick)
        return rows

    def send(k, value):
        for h in range(2):
            frame[k, h] = value[h]
        for peer in peers:
            pltpu.make_async_remote_copy(
                src_ref=frame.at[k],
                dst_ref=planes.at[k, here, :, pl.ds(pair, 1), :],
                send_sem=send_sem.at[k],
                recv_sem=recv_sem.at[k],
                device_id=peer,
                device_id_type=LOGICAL,
            ).start()
        for h in range(2):
            planes[k, here, h, pl.ds(pair, 1), :] = value[h]

    def counted(sem):
        done = slots.at[:]
        return pltpu.make_async_copy(done, done, sem)

    def receive(k):
        counted(recv_sem.at[k]).wait()
        part = [planes[k, 0, h] + planes[k, 1, h] for h in range(2)]
        rest = [planes[k, 2, h] + planes[k, 3, h] for h in range(2)]
        rows = [part[0], part[1] + rest[0], rest[1]]
        for j in range(3):
            x_rows[j] = rows[j]
        return jnp.concatenate(rows, axis=0)

    def own_rows():
        return [x_rows[odd + h, pl.ds(pair, 1), :] for h in range(2)]

    def multiply(diag):
        own = own_rows()
        acc = [None] * (ROWS // 8)
        for n in range(COLS // LANES):
            value = x_rows[n % 3, pl.ds(col * (PAIRS // 2) + n // 3, 1), :]
            wide = jnp.broadcast_to(value, (8, LANES))
            for g in range(ROWS // 8):
                term = mat[8 * g : 8 * g + 8, n * LANES : (n + 1) * LANES] * wide
                acc[g] = term if n == 0 else acc[g] + term
        zero = jnp.zeros((8, LANES), jnp.float32)
        is_odd = odd == 1
        padded = [
            jnp.where(is_odd, acc[t - 8] if t >= 8 else zero, acc[t] if t < 24 else zero) for t in range(32)
        ]
        rows = []
        for h in range(2):
            block = jnp.concatenate(padded[16 * h : 16 * h + 16], axis=0)
            rows.append(jnp.sum(block.T, axis=0, keepdims=True) + diag[h] * own[h])
        return rows

    def unframed(first, second):
        pick = None
        for o in range(2):
            for c in range(2):
                offset = 64 * o + TILE * c
                shift = offset % LANES
                if offset >= LANES:
                    moved = pltpu.roll(second, LANES - shift, 1)
                elif shift:
                    moved = pltpu.roll(jnp.where(lane >= shift, first, second), LANES - shift, 1)
                else:
                    moved = first
                pick = moved if pick is None else jnp.where(here == 2 * o + c, moved, pick)
        return pick

    load_start.wait()
    first = framed(small[0])
    load_diag.wait()
    diag = framed(small[1])
    pl.semaphore_wait(barrier, DEVICES - 1)
    send(0, first)
    load.wait()

    scale = jnp.float32(math.sqrt(DIM))
    known, images, slices = [], [], []
    for k in range(ITERS + 1):
        vector = receive(k)
        own = unframed(*own_rows())
        if k < ITERS:
            image = multiply(diag)
        dots = [total(q * vector) for q in known]
        for h, q, s in zip(dots, known, slices):
            vector = vector - h * q
            own = own - h * s
        norm = jnp.sqrt(total(vector * vector))
        if k < ITERS:
            for h, f in zip(dots, images):
                image = [a - h * b for a, b in zip(image, f)]
            image = [a / norm for a in image]
            send(k + 1, image)
            images.append(image)
            known.append(vector / norm)
        own = own / norm
        slices.append(own)
        out[k : k + 1, :] = own * scale
        if k:
            column = lane == k - 1
            a_row = jnp.where(column, dots[-1], a_row if k > 1 else 0.0)
            b_row = jnp.where(column, norm, b_row if k > 1 else 0.0)
    out[4:5, :] = a_row
    out[5:6, :] = b_row
    for k in range(ITERS + 1):
        counted(send_sem.at[k]).wait()


def split_kernel(packed, basis, coef):
    basis[...] = packed[0:4, 0:TILE]
    coef[...] = packed[4:6, 0:ITERS]


def solution(mesh):
    vmem = pl.BlockSpec(memory_space=pltpu.VMEM)
    hbm = pl.BlockSpec(memory_space=pl.ANY)

    def local(matrix, diagonal, start):
        packed = pl.pallas_call(
            kernel,
            out_shape=pltpu.VMEM((8, LANES), jnp.float32),
            in_specs=[hbm, hbm, hbm],
            out_specs=vmem,
            scratch_shapes=[
                pltpu.VMEM((ROWS, COLS), jnp.float32),
                pltpu.VMEM((2, 1, TILE), jnp.float32),
                pltpu.VMEM((ITERS + 1, 2, 1, LANES), jnp.float32),
                pltpu.VMEM((ITERS + 1, 4, 2, PAIRS, LANES), jnp.float32),
                pltpu.VMEM((3, PAIRS, LANES), jnp.float32),
                pltpu.VMEM((DEVICES - 1, 2, LANES), jnp.float32),
                pltpu.SemaphoreType.DMA,
                pltpu.SemaphoreType.DMA((2,)),
                pltpu.SemaphoreType.DMA((ITERS + 1,)),
                pltpu.SemaphoreType.DMA((ITERS + 1,)),
            ],
            compiler_params=pltpu.CompilerParams(collective_id=0, has_side_effects=True),
        )(matrix, diagonal.reshape(1, TILE), start.reshape(1, TILE))
        return pl.pallas_call(
            split_kernel,
            out_shape=(
                jax.ShapeDtypeStruct((ITERS + 1, TILE), jnp.float32),
                jax.ShapeDtypeStruct((2, ITERS), jnp.float32),
            ),
            in_specs=[vmem],
            out_specs=(vmem, vmem),
        )(pltpu.with_memory_space_constraint(packed, pltpu.VMEM))

    return jax.shard_map(
        local,
        mesh=mesh,
        in_specs=(P("row", "col"), P(("row", "col")), P(("row", "col"))),
        out_specs=(P(None, ("row", "col")), P()),
        check_vma=False,
    )
```

```python
import math

import jax
import jax.numpy as jnp
from jax import lax
from jax.experimental import pallas as pl
from jax.experimental.pallas import tpu as pltpu
from jax.sharding import PartitionSpec as P

ITERS = 3
DIM = 12288
DEVICES = 128
ROWS = 192
COLS = 6144
TILE = 96
LANES = 128
PAIRS = 32
LOGICAL = pl.DeviceIdType.LOGICAL


def hops(step):
    return (0, 1, 2, 1)[step]


STEPS = sorted(
    (
        (i, j, k, m)
        for i in range(4)
        for j in range(4)
        for k in range(4)
        for m in range(2)
        if i or j or k
    ),
    key=lambda s: (-(hops(s[0]) + hops(s[1]) + hops(s[2])), s[3]),
)


def total(value):
    return jnp.sum(value, keepdims=True)


def kernel(matrix, diagonal, start, out, mat, small, frame, planes, x_rows, slots, mat_sem, small_sem, send_sem, recv_sem):
    row = lax.axis_index("row")
    col = lax.axis_index("col")
    pair = row // 2
    odd = row % 2
    here = odd * 2 + col
    slot = here * 2 * PAIRS + pair * 2
    z, y, x = row // 16, (row // 4) % 4, row % 4
    z_part = [((z + i) % 4) * 32 for i in range(4)]
    y_part = [((y + i) % 4) * 8 for i in range(4)]
    x_part = [((x + i) % 4) * 2 for i in range(4)]
    peers = [z_part[i] + y_part[j] + x_part[k] + m for i, j, k, m in STEPS]
    peers.append(row * 2 + 1 - col)

    barrier = pltpu.get_barrier_semaphore()
    for peer in peers:
        pl.semaphore_signal(barrier, inc=1, device_id=peer, device_id_type=LOGICAL)
    load_start = pltpu.make_async_copy(start, small.at[0], small_sem.at[0])
    load_diag = pltpu.make_async_copy(diagonal, small.at[1], small_sem.at[1])
    load = pltpu.make_async_copy(matrix, mat, mat_sem)
    load_start.start()
    load_diag.start()
    load.start()

    lane = lax.broadcasted_iota(jnp.int32, (1, LANES), 1)

    def framed(part):
        wide = jnp.concatenate([part, jnp.zeros((1, LANES - TILE), jnp.float32)], axis=1)
        out = []
        for o in range(2):
            for c in range(2):
                offset = 64 * o + TILE * c
                shift = offset % LANES
                moved = pltpu.roll(wide, shift, 1) if shift else wide
                first, second = jnp.where(lane >= shift, moved, 0.0), jnp.where(lane < shift, moved, 0.0)
                zero = jnp.zeros_like(moved)
                out.append((zero, first) if offset >= LANES else (first, second))
        rows = []
        for h in range(2):
            pick = out[0][h]
            for n in range(1, 4):
                pick = jnp.where(here == n, out[n][h], pick)
            rows.append(pick)
        return rows

    def send(k, value):
        for h in range(2):
            frame[k, h : h + 1, :] = value[h]
        for peer in peers:
            pltpu.make_async_remote_copy(
                src_ref=frame.at[k],
                dst_ref=planes.at[k, pl.ds(slot, 2), :],
                send_sem=send_sem.at[k],
                recv_sem=recv_sem.at[k],
                device_id=peer,
                device_id_type=LOGICAL,
            ).start()
        for h in range(2):
            planes[k, pl.ds(slot + h, 1), :] = value[h]

    def counted(sem):
        done = slots.at[:]
        return pltpu.make_async_copy(done, done, sem)

    def receive(k):
        counted(recv_sem.at[k]).wait()
        side = [
            [planes[k, pl.ds(2 * PAIRS * n + h, PAIRS, stride=2), :] for h in range(2)] for n in range(4)
        ]
        part = [side[0][h] + side[1][h] for h in range(2)]
        rest = [side[2][h] + side[3][h] for h in range(2)]
        rows = [part[0], part[1] + rest[0], rest[1]]
        for j in range(3):
            x_rows[j] = rows[j]
        return jnp.concatenate(rows, axis=0)

    def own_rows():
        return [x_rows[odd + h, pl.ds(pair, 1), :] for h in range(2)]

    def multiply(diag):
        own = own_rows()
        acc = [None] * (ROWS // 8)
        for n in range(COLS // LANES):
            value = x_rows[n % 3, pl.ds(col * (PAIRS // 2) + n // 3, 1), :]
            wide = jnp.broadcast_to(value, (8, LANES))
            for g in range(ROWS // 8):
                term = mat[8 * g : 8 * g + 8, n * LANES : (n + 1) * LANES] * wide
                acc[g] = term if n == 0 else acc[g] + term
        zero = jnp.zeros((8, LANES), jnp.float32)
        is_odd = odd == 1
        padded = [
            jnp.where(is_odd, acc[t - 8] if t >= 8 else zero, acc[t] if t < 24 else zero) for t in range(32)
        ]
        rows = []
        for h in range(2):
            block = jnp.concatenate(padded[16 * h : 16 * h + 16], axis=0)
            rows.append(jnp.sum(block.T, axis=0, keepdims=True) + diag[h] * own[h])
        return rows

    def unframed(first, second):
        pick = None
        for o in range(2):
            for c in range(2):
                offset = 64 * o + TILE * c
                shift = offset % LANES
                if offset >= LANES:
                    moved = pltpu.roll(second, LANES - shift, 1)
                elif shift:
                    moved = pltpu.roll(jnp.where(lane >= shift, first, second), LANES - shift, 1)
                else:
                    moved = first
                pick = moved if pick is None else jnp.where(here == 2 * o + c, moved, pick)
        return pick

    load_start.wait()
    first = framed(small[0])
    load_diag.wait()
    diag = framed(small[1])
    pl.semaphore_wait(barrier, DEVICES - 1)
    send(0, first)
    load.wait()

    scale = jnp.float32(math.sqrt(DIM))
    known, images, slices = [], [], []
    for k in range(ITERS + 1):
        vector = receive(k)
        own = unframed(*own_rows())
        if k < ITERS:
            image = multiply(diag)
        dots = [total(q * vector) for q in known]
        for h, q, s in zip(dots, known, slices):
            vector = vector - h * q
            own = own - h * s
        norm = jnp.sqrt(total(vector * vector))
        if k < ITERS:
            for h, f in zip(dots, images):
                image = [a - h * b for a, b in zip(image, f)]
            image = [a / norm for a in image]
            send(k + 1, image)
            images.append(image)
            known.append(vector / norm)
        own = own / norm
        slices.append(own)
        out[k : k + 1, :] = own * scale
        if k:
            column = lane == k - 1
            a_row = jnp.where(column, dots[-1], a_row if k > 1 else 0.0)
            b_row = jnp.where(column, norm, b_row if k > 1 else 0.0)
    out[4:5, :] = a_row
    out[5:6, :] = b_row
    for k in range(ITERS + 1):
        counted(send_sem.at[k]).wait()


def split_kernel(packed, basis, coef):
    basis[...] = packed[0:4, 0:TILE]
    coef[...] = packed[4:6, 0:ITERS]


def solution(mesh):
    vmem = pl.BlockSpec(memory_space=pltpu.VMEM)
    hbm = pl.BlockSpec(memory_space=pl.ANY)

    def local(matrix, diagonal, start):
        packed = pl.pallas_call(
            kernel,
            out_shape=pltpu.VMEM((8, LANES), jnp.float32),
            in_specs=[hbm, hbm, hbm],
            out_specs=vmem,
            scratch_shapes=[
                pltpu.VMEM((ROWS, COLS), jnp.float32),
                pltpu.VMEM((2, 1, TILE), jnp.float32),
                pltpu.VMEM((ITERS + 1, 2, LANES), jnp.float32),
                pltpu.VMEM((ITERS + 1, 8 * PAIRS, LANES), jnp.float32),
                pltpu.VMEM((3, PAIRS, LANES), jnp.float32),
                pltpu.VMEM((DEVICES - 1, 2, LANES), jnp.float32),
                pltpu.SemaphoreType.DMA,
                pltpu.SemaphoreType.DMA((2,)),
                pltpu.SemaphoreType.DMA((ITERS + 1,)),
                pltpu.SemaphoreType.DMA((ITERS + 1,)),
            ],
            compiler_params=pltpu.CompilerParams(collective_id=0, has_side_effects=True),
        )(matrix, diagonal.reshape(1, TILE), start.reshape(1, TILE))
        return pl.pallas_call(
            split_kernel,
            out_shape=(
                jax.ShapeDtypeStruct((ITERS + 1, TILE), jnp.float32),
                jax.ShapeDtypeStruct((2, ITERS), jnp.float32),
            ),
            in_specs=[vmem],
            out_specs=(vmem, vmem),
        )(pltpu.with_memory_space_constraint(packed, pltpu.VMEM))

    return jax.shard_map(
        local,
        mesh=mesh,
        in_specs=(P("row", "col"), P(("row", "col")), P(("row", "col"))),
        out_specs=(P(None, ("row", "col")), P()),
        check_vma=False,
    )
```

```python
import math

import jax
import jax.numpy as jnp
from jax import lax
from jax.experimental import pallas as pl
from jax.experimental.pallas import tpu as pltpu
from jax.sharding import PartitionSpec as P

ITERS = 3
DIM = 12288
DEVICES = 128
ROWS = 192
COLS = 6144
TILE = 96
LANES = 128
PAIRS = 32
LOGICAL = pl.DeviceIdType.LOGICAL


def hops(step):
    return (0, 1, 2, 1)[step]


STEPS = sorted(
    (
        (i, j, k, m)
        for i in range(4)
        for j in range(4)
        for k in range(4)
        for m in range(2)
        if i or j or k
    ),
    key=lambda s: (-(hops(s[0]) + hops(s[1]) + hops(s[2])), s[3]),
)


def total(value):
    return jnp.sum(value, keepdims=True)


def kernel(matrix, diagonal, start, out, mat, small, frame, planes, x_rows, slots, mat_sem, small_sem, send_sem, recv_sem):
    row = lax.axis_index("row")
    col = lax.axis_index("col")
    pair = row // 2
    odd = row % 2
    here = odd * 2 + col
    slot = here * 2 * PAIRS + pair * 2
    z, y, x = row // 16, (row // 4) % 4, row % 4
    z_part = [((z + i) % 4) * 32 for i in range(4)]
    y_part = [((y + i) % 4) * 8 for i in range(4)]
    x_part = [((x + i) % 4) * 2 for i in range(4)]
    peers = [z_part[i] + y_part[j] + x_part[k] + m for i, j, k, m in STEPS]
    peers.append(row * 2 + 1 - col)

    barrier = pltpu.get_barrier_semaphore()
    for peer in peers:
        pl.semaphore_signal(barrier, inc=1, device_id=peer, device_id_type=LOGICAL)
    load_start = pltpu.make_async_copy(start, small.at[0], small_sem.at[0])
    load_diag = pltpu.make_async_copy(diagonal, small.at[1], small_sem.at[1])
    load = pltpu.make_async_copy(matrix, mat, mat_sem)
    load_start.start()
    load_diag.start()
    load.start()

    lane = lax.broadcasted_iota(jnp.int32, (1, LANES), 1)

    def framed(part):
        wide = jnp.concatenate([part, jnp.zeros((1, LANES - TILE), jnp.float32)], axis=1)
        out = []
        for o in range(2):
            for c in range(2):
                offset = 64 * o + TILE * c
                shift = offset % LANES
                moved = pltpu.roll(wide, shift, 1) if shift else wide
                first, second = jnp.where(lane >= shift, moved, 0.0), jnp.where(lane < shift, moved, 0.0)
                zero = jnp.zeros_like(moved)
                out.append((zero, first) if offset >= LANES else (first, second))
        rows = []
        for h in range(2):
            pick = out[0][h]
            for n in range(1, 4):
                pick = jnp.where(here == n, out[n][h], pick)
            rows.append(pick)
        return rows

    def send(k, value):
        for h in range(2):
            frame[k, h : h + 1, :] = value[h]
        for peer in peers:
            pltpu.make_async_remote_copy(
                src_ref=frame.at[k],
                dst_ref=planes.at[k, pl.ds(slot, 2), :],
                send_sem=send_sem.at[k],
                recv_sem=recv_sem.at[k],
                device_id=peer,
                device_id_type=LOGICAL,
            ).start()
        for h in range(2):
            planes[k, pl.ds(slot + h, 1), :] = value[h]

    def counted(sem):
        done = slots.at[:]
        return pltpu.make_async_copy(done, done, sem)

    def receive(k):
        counted(recv_sem.at[k]).wait()
        side = [
            [planes[k, pl.ds(2 * PAIRS * n + h, PAIRS, stride=2), :] for h in range(2)] for n in range(4)
        ]
        part = [side[0][h] + side[1][h] for h in range(2)]
        rest = [side[2][h] + side[3][h] for h in range(2)]
        rows = [part[0], part[1] + rest[0], rest[1]]
        for j in range(3):
            x_rows[j] = rows[j]
        return jnp.concatenate(rows, axis=0)

    def own_rows():
        return [x_rows[odd + h, pl.ds(pair, 1), :] for h in range(2)]

    def multiply(diag):
        own = own_rows()
        acc = [None] * (ROWS // 8)
        for groups in (range(8), range(8, 16), range(16, 24)):
            for n in range(COLS // LANES):
                value = x_rows[n % 3, pl.ds(col * (PAIRS // 2) + n // 3, 1), :]
                wide = jnp.broadcast_to(value, (8, LANES))
                for g in groups:
                    term = mat[8 * g : 8 * g + 8, n * LANES : (n + 1) * LANES] * wide
                    acc[g] = term if n == 0 else acc[g] + term
        zero = jnp.zeros((8, LANES), jnp.float32)
        is_odd = odd == 1
        padded = [
            jnp.where(is_odd, acc[t - 8] if t >= 8 else zero, acc[t] if t < 24 else zero) for t in range(32)
        ]
        rows = []
        for h in range(2):
            block = jnp.concatenate(padded[16 * h : 16 * h + 16], axis=0)
            rows.append(jnp.sum(block.T, axis=0, keepdims=True) + diag[h] * own[h])
        return rows

    def unframed(first, second):
        pick = None
        for o in range(2):
            for c in range(2):
                offset = 64 * o + TILE * c
                shift = offset % LANES
                if offset >= LANES:
                    moved = pltpu.roll(second, LANES - shift, 1)
                elif shift:
                    moved = pltpu.roll(jnp.where(lane >= shift, first, second), LANES - shift, 1)
                else:
                    moved = first
                pick = moved if pick is None else jnp.where(here == 2 * o + c, moved, pick)
        return pick

    load_start.wait()
    first = framed(small[0])
    load_diag.wait()
    diag = framed(small[1])
    pl.semaphore_wait(barrier, DEVICES - 1)
    send(0, first)
    load.wait()

    scale = jnp.float32(math.sqrt(DIM))
    known, images, slices = [], [], []
    for k in range(ITERS + 1):
        vector = receive(k)
        own = unframed(*own_rows())
        if k < ITERS:
            image = multiply(diag)
        dots = [total(q * vector) for q in known]
        for h, q, s in zip(dots, known, slices):
            vector = vector - h * q
            own = own - h * s
        norm = jnp.sqrt(total(vector * vector))
        if k < ITERS:
            for h, f in zip(dots, images):
                image = [a - h * b for a, b in zip(image, f)]
            image = [a / norm for a in image]
            send(k + 1, image)
            images.append(image)
            known.append(vector / norm)
        own = own / norm
        slices.append(own)
        out[k : k + 1, :] = own * scale
        if k:
            column = lane == k - 1
            a_row = jnp.where(column, dots[-1], a_row if k > 1 else 0.0)
            b_row = jnp.where(column, norm, b_row if k > 1 else 0.0)
    out[4:5, :] = a_row
    out[5:6, :] = b_row
    for k in range(ITERS + 1):
        counted(send_sem.at[k]).wait()


def split_kernel(packed, basis, coef):
    basis[...] = packed[0:4, 0:TILE]
    coef[...] = packed[4:6, 0:ITERS]


def solution(mesh):
    vmem = pl.BlockSpec(memory_space=pltpu.VMEM)
    hbm = pl.BlockSpec(memory_space=pl.ANY)

    def local(matrix, diagonal, start):
        packed = pl.pallas_call(
            kernel,
            out_shape=pltpu.VMEM((8, LANES), jnp.float32),
            in_specs=[hbm, hbm, hbm],
            out_specs=vmem,
            scratch_shapes=[
                pltpu.VMEM((ROWS, COLS), jnp.float32),
                pltpu.VMEM((2, 1, TILE), jnp.float32),
                pltpu.VMEM((ITERS + 1, 2, LANES), jnp.float32),
                pltpu.VMEM((ITERS + 1, 8 * PAIRS, LANES), jnp.float32),
                pltpu.VMEM((3, PAIRS, LANES), jnp.float32),
                pltpu.VMEM((DEVICES - 1, 2, LANES), jnp.float32),
                pltpu.SemaphoreType.DMA,
                pltpu.SemaphoreType.DMA((2,)),
                pltpu.SemaphoreType.DMA((ITERS + 1,)),
                pltpu.SemaphoreType.DMA((ITERS + 1,)),
            ],
            compiler_params=pltpu.CompilerParams(collective_id=0, has_side_effects=True),
        )(matrix, diagonal.reshape(1, TILE), start.reshape(1, TILE))
        return pl.pallas_call(
            split_kernel,
            out_shape=(
                jax.ShapeDtypeStruct((ITERS + 1, TILE), jnp.float32),
                jax.ShapeDtypeStruct((2, ITERS), jnp.float32),
            ),
            in_specs=[vmem],
            out_specs=(vmem, vmem),
        )(pltpu.with_memory_space_constraint(packed, pltpu.VMEM))

    return jax.shard_map(
        local,
        mesh=mesh,
        in_specs=(P("row", "col"), P(("row", "col")), P(("row", "col"))),
        out_specs=(P(None, ("row", "col")), P()),
        check_vma=False,
    )
```

```python
import math

import jax
import jax.numpy as jnp
from jax import lax
from jax.experimental import pallas as pl
from jax.experimental.pallas import tpu as pltpu
from jax.sharding import PartitionSpec as P

ITERS = 3
DIM = 12288
DEVICES = 128
ROWS = 192
COLS = 6144
TILE = 96
LANES = 128
PAIRS = 32
LOGICAL = pl.DeviceIdType.LOGICAL


def hops(step):
    return (0, 1, 2, 1)[step]


STEPS = sorted(
    (
        (i, j, k, m)
        for i in range(4)
        for j in range(4)
        for k in range(4)
        for m in range(2)
        if i or j or k
    ),
    key=lambda s: (-(hops(s[0]) + hops(s[1]) + hops(s[2])), s[3]),
)


def total(value):
    return jnp.sum(value, keepdims=True)


def kernel(matrix, diagonal, start, out, mat, small, frame, planes, x_rows, slots, mat_sem, small_sem, send_sem, recv_sem):
    row = lax.axis_index("row")
    col = lax.axis_index("col")
    pair = row // 2
    odd = row % 2
    here = odd * 2 + col
    slot = here * 2 * PAIRS + pair * 2
    z, y, x = row // 16, (row // 4) % 4, row % 4
    z_part = [((z + i) % 4) * 32 for i in range(4)]
    y_part = [((y + i) % 4) * 8 for i in range(4)]
    x_part = [((x + i) % 4) * 2 for i in range(4)]
    peers = [z_part[i] + y_part[j] + x_part[k] + m for i, j, k, m in STEPS]
    peers.append(row * 2 + 1 - col)

    barrier = pltpu.get_barrier_semaphore()
    for peer in peers:
        pl.semaphore_signal(barrier, inc=1, device_id=peer, device_id_type=LOGICAL)
    load_start = pltpu.make_async_copy(start, small.at[0], small_sem.at[0])
    load_diag = pltpu.make_async_copy(diagonal, small.at[1], small_sem.at[1])
    load = pltpu.make_async_copy(matrix, mat, mat_sem)
    load_start.start()
    load_diag.start()
    load.start()

    lane = lax.broadcasted_iota(jnp.int32, (1, LANES), 1)

    def framed(part):
        wide = jnp.concatenate([part, jnp.zeros((1, LANES - TILE), jnp.float32)], axis=1)
        out = []
        for o in range(2):
            for c in range(2):
                offset = 64 * o + TILE * c
                shift = offset % LANES
                moved = pltpu.roll(wide, shift, 1) if shift else wide
                first, second = jnp.where(lane >= shift, moved, 0.0), jnp.where(lane < shift, moved, 0.0)
                zero = jnp.zeros_like(moved)
                out.append((zero, first) if offset >= LANES else (first, second))
        rows = []
        for h in range(2):
            pick = out[0][h]
            for n in range(1, 4):
                pick = jnp.where(here == n, out[n][h], pick)
            rows.append(pick)
        return rows

    def send(k, value):
        for h in range(2):
            frame[k, h : h + 1, :] = value[h]
        for peer in peers:
            pltpu.make_async_remote_copy(
                src_ref=frame.at[k],
                dst_ref=planes.at[k, pl.ds(slot, 2), :],
                send_sem=send_sem.at[k],
                recv_sem=recv_sem.at[k],
                device_id=peer,
                device_id_type=LOGICAL,
            ).start()
        for h in range(2):
            planes[k, pl.ds(slot + h, 1), :] = value[h]

    def counted(sem):
        done = slots.at[:]
        return pltpu.make_async_copy(done, done, sem)

    def receive(k):
        counted(recv_sem.at[k]).wait()
        side = [
            [planes[k, pl.ds(2 * PAIRS * n + h, PAIRS, stride=2), :] for h in range(2)] for n in range(4)
        ]
        part = [side[0][h] + side[1][h] for h in range(2)]
        rest = [side[2][h] + side[3][h] for h in range(2)]
        rows = [part[0], part[1] + rest[0], rest[1]]
        for j in range(3):
            x_rows[j] = rows[j]
        return jnp.concatenate(rows, axis=0)

    def own_rows():
        return [x_rows[odd + h, pl.ds(pair, 1), :] for h in range(2)]

    def multiply(diag):
        own = own_rows()
        acc = [None] * (ROWS // 8)
        for groups in (range(8), range(8, 16), range(16, 24)):
            for n in range(COLS // LANES):
                value = x_rows[n % 3, pl.ds(col * (PAIRS // 2) + n // 3, 1), :]
                wide = jnp.broadcast_to(value, (8, LANES))
                for g in groups:
                    term = mat[8 * g : 8 * g + 8, n * LANES : (n + 1) * LANES] * wide
                    acc[g] = term if n == 0 else acc[g] + term
        zero = jnp.zeros((8, LANES), jnp.float32)
        is_odd = odd == 1
        padded = [
            jnp.where(is_odd, acc[t - 8] if t >= 8 else zero, acc[t] if t < 24 else zero) for t in range(32)
        ]
        rows = []
        for h in range(2):
            block = jnp.concatenate(padded[16 * h : 16 * h + 16], axis=0)
            rows.append(jnp.sum(block.T, axis=0, keepdims=True) + diag[h] * own[h])
        return rows

    def unframed(first, second):
        pick = None
        for o in range(2):
            for c in range(2):
                offset = 64 * o + TILE * c
                shift = offset % LANES
                if offset >= LANES:
                    moved = pltpu.roll(second, LANES - shift, 1)
                elif shift:
                    moved = pltpu.roll(jnp.where(lane >= shift, first, second), LANES - shift, 1)
                else:
                    moved = first
                pick = moved if pick is None else jnp.where(here == 2 * o + c, moved, pick)
        return pick

    load_start.wait()
    first = framed(small[0])
    load_diag.wait()
    diag = framed(small[1])
    pl.semaphore_wait(barrier, DEVICES - 1)
    send(0, first)
    load.wait()

    scale = jnp.float32(math.sqrt(DIM))
    known, images, slices = [], [], []
    for k in range(ITERS + 1):
        vector = receive(k)
        own = unframed(*own_rows())
        if k < ITERS:
            image = multiply(diag)
        dots = [total(q * vector) for q in known]
        for h, q, s in zip(dots, known, slices):
            vector = vector - h * q
            own = own - h * s
        norm = jnp.sqrt(total(vector * vector))
        if k < ITERS:
            for h, f in zip(dots, images):
                image = [a - h * b for a, b in zip(image, f)]
            image = [a / norm for a in image]
            send(k + 1, image)
            counted(send_sem.at[k]).wait()
            images.append(image)
            known.append(vector / norm)
        own = own / norm
        slices.append(own)
        out[k : k + 1, :] = own * scale
        if k:
            column = lane == k - 1
            a_row = jnp.where(column, dots[-1], a_row if k > 1 else 0.0)
            b_row = jnp.where(column, norm, b_row if k > 1 else 0.0)
    out[4:5, :] = a_row
    out[5:6, :] = b_row
    counted(send_sem.at[ITERS]).wait()


def split_kernel(packed, basis, coef):
    basis[...] = packed[0:4, 0:TILE]
    coef[...] = packed[4:6, 0:ITERS]


def solution(mesh):
    vmem = pl.BlockSpec(memory_space=pltpu.VMEM)
    hbm = pl.BlockSpec(memory_space=pl.ANY)

    def local(matrix, diagonal, start):
        packed = pl.pallas_call(
            kernel,
            out_shape=pltpu.VMEM((8, LANES), jnp.float32),
            in_specs=[hbm, hbm, hbm],
            out_specs=vmem,
            scratch_shapes=[
                pltpu.VMEM((ROWS, COLS), jnp.float32),
                pltpu.VMEM((2, 1, TILE), jnp.float32),
                pltpu.VMEM((ITERS + 1, 2, LANES), jnp.float32),
                pltpu.VMEM((ITERS + 1, 8 * PAIRS, LANES), jnp.float32),
                pltpu.VMEM((3, PAIRS, LANES), jnp.float32),
                pltpu.VMEM((DEVICES - 1, 2, LANES), jnp.float32),
                pltpu.SemaphoreType.DMA,
                pltpu.SemaphoreType.DMA((2,)),
                pltpu.SemaphoreType.DMA((ITERS + 1,)),
                pltpu.SemaphoreType.DMA((ITERS + 1,)),
            ],
            compiler_params=pltpu.CompilerParams(collective_id=0, has_side_effects=True),
        )(matrix, diagonal.reshape(1, TILE), start.reshape(1, TILE))
        return pl.pallas_call(
            split_kernel,
            out_shape=(
                jax.ShapeDtypeStruct((ITERS + 1, TILE), jnp.float32),
                jax.ShapeDtypeStruct((2, ITERS), jnp.float32),
            ),
            in_specs=[vmem],
            out_specs=(vmem, vmem),
        )(pltpu.with_memory_space_constraint(packed, pltpu.VMEM))

    return jax.shard_map(
        local,
        mesh=mesh,
        in_specs=(P("row", "col"), P(("row", "col")), P(("row", "col"))),
        out_specs=(P(None, ("row", "col")), P()),
        check_vma=False,
    )
```

```python
import math

import jax
import jax.numpy as jnp
from jax import lax
from jax.experimental import pallas as pl
from jax.experimental.pallas import tpu as pltpu
from jax.sharding import PartitionSpec as P

ITERS = 3
DIM = 12288
DEVICES = 128
ROWS = 192
COLS = 6144
TILE = 96
LANES = 128
PAIRS = 32
LOGICAL = pl.DeviceIdType.LOGICAL


def hops(step):
    return (0, 1, 2, 1)[step]


STEPS = sorted(
    (
        (i, j, k, m)
        for i in range(4)
        for j in range(4)
        for k in range(4)
        for m in range(2)
        if i or j or k
    ),
    key=lambda s: (-(hops(s[0]) + hops(s[1]) + hops(s[2])), s[3]),
)


def total(value):
    return jnp.sum(value, keepdims=True)


def kernel(matrix, diagonal, start, out, mat, small, frame, planes, x_rows, slots, mat_sem, small_sem, send_sem, recv_sem):
    row = lax.axis_index("row")
    col = lax.axis_index("col")
    pair = row // 2
    odd = row % 2
    here = odd * 2 + col
    slot = here * 2 * PAIRS + pair * 2
    z, y, x = row // 16, (row // 4) % 4, row % 4
    z_part = [((z + i) % 4) * 32 for i in range(4)]
    y_part = [((y + i) % 4) * 8 for i in range(4)]
    x_part = [((x + i) % 4) * 2 for i in range(4)]
    peers = [z_part[i] + y_part[j] + x_part[k] + m for i, j, k, m in STEPS]
    peers.append(row * 2 + 1 - col)

    barrier = pltpu.get_barrier_semaphore()
    for peer in peers:
        pl.semaphore_signal(barrier, inc=1, device_id=peer, device_id_type=LOGICAL)
    load_start = pltpu.make_async_copy(start, small.at[0], small_sem.at[0])
    load_diag = pltpu.make_async_copy(diagonal, small.at[1], small_sem.at[1])
    load = pltpu.make_async_copy(matrix, mat, mat_sem)
    load_start.start()
    load_diag.start()
    load.start()

    lane = lax.broadcasted_iota(jnp.int32, (1, LANES), 1)

    def framed(part):
        wide = jnp.concatenate([part, jnp.zeros((1, LANES - TILE), jnp.float32)], axis=1)
        out = []
        for o in range(2):
            for c in range(2):
                offset = 64 * o + TILE * c
                shift = offset % LANES
                moved = pltpu.roll(wide, shift, 1) if shift else wide
                first, second = jnp.where(lane >= shift, moved, 0.0), jnp.where(lane < shift, moved, 0.0)
                zero = jnp.zeros_like(moved)
                out.append((zero, first) if offset >= LANES else (first, second))
        rows = []
        for h in range(2):
            pick = out[0][h]
            for n in range(1, 4):
                pick = jnp.where(here == n, out[n][h], pick)
            rows.append(pick)
        return rows

    def send(k, value):
        for h in range(2):
            frame[k, h : h + 1, :] = value[h]
        for peer in peers:
            pltpu.make_async_remote_copy(
                src_ref=frame.at[k],
                dst_ref=planes.at[k, pl.ds(slot, 2), :],
                send_sem=send_sem.at[k],
                recv_sem=recv_sem.at[k],
                device_id=peer,
                device_id_type=LOGICAL,
            ).start()
        for h in range(2):
            planes[k, pl.ds(slot + h, 1), :] = value[h]

    def counted(sem):
        done = slots.at[:]
        return pltpu.make_async_copy(done, done, sem)

    def receive(k):
        counted(recv_sem.at[k]).wait()
        side = [
            [planes[k, pl.ds(2 * PAIRS * n + h, PAIRS, stride=2), :] for h in range(2)] for n in range(4)
        ]
        part = [side[0][h] + side[1][h] for h in range(2)]
        rest = [side[2][h] + side[3][h] for h in range(2)]
        rows = [part[0], part[1] + rest[0], rest[1]]
        for j in range(3):
            x_rows[j] = rows[j]
        return jnp.concatenate(rows, axis=0)

    def own_rows():
        return [x_rows[odd + h, pl.ds(pair, 1), :] for h in range(2)]

    def multiply(diag):
        own = own_rows()
        acc = [None] * (ROWS // 8)
        for groups in (range(12), range(12, 24)):
            for n in range(COLS // LANES):
                value = x_rows[n % 3, pl.ds(col * (PAIRS // 2) + n // 3, 1), :]
                wide = jnp.broadcast_to(value, (8, LANES))
                for g in groups:
                    term = mat[8 * g : 8 * g + 8, n * LANES : (n + 1) * LANES] * wide
                    acc[g] = term if n == 0 else acc[g] + term
        zero = jnp.zeros((8, LANES), jnp.float32)
        is_odd = odd == 1
        padded = [
            jnp.where(is_odd, acc[t - 8] if t >= 8 else zero, acc[t] if t < 24 else zero) for t in range(32)
        ]
        rows = []
        for h in range(2):
            block = jnp.concatenate(padded[16 * h : 16 * h + 16], axis=0)
            rows.append(jnp.sum(block.T, axis=0, keepdims=True) + diag[h] * own[h])
        return rows

    def unframed(first, second):
        pick = None
        for o in range(2):
            for c in range(2):
                offset = 64 * o + TILE * c
                shift = offset % LANES
                if offset >= LANES:
                    moved = pltpu.roll(second, LANES - shift, 1)
                elif shift:
                    moved = pltpu.roll(jnp.where(lane >= shift, first, second), LANES - shift, 1)
                else:
                    moved = first
                pick = moved if pick is None else jnp.where(here == 2 * o + c, moved, pick)
        return pick

    load_start.wait()
    first = framed(small[0])
    load_diag.wait()
    diag = framed(small[1])
    pl.semaphore_wait(barrier, DEVICES - 1)
    send(0, first)
    load.wait()

    scale = jnp.float32(math.sqrt(DIM))
    known, images, slices = [], [], []
    for k in range(ITERS + 1):
        vector = receive(k)
        own = unframed(*own_rows())
        if k < ITERS:
            image = multiply(diag)
        dots = [total(q * vector) for q in known]
        for h, q, s in zip(dots, known, slices):
            vector = vector - h * q
            own = own - h * s
        norm = jnp.sqrt(total(vector * vector))
        if k < ITERS:
            for h, f in zip(dots, images):
                image = [a - h * b for a, b in zip(image, f)]
            image = [a / norm for a in image]
            send(k + 1, image)
            counted(send_sem.at[k]).wait()
            images.append(image)
            known.append(vector / norm)
        own = own / norm
        slices.append(own)
        out[k : k + 1, :] = own * scale
        if k:
            column = lane == k - 1
            a_row = jnp.where(column, dots[-1], a_row if k > 1 else 0.0)
            b_row = jnp.where(column, norm, b_row if k > 1 else 0.0)
    out[4:5, :] = a_row
    out[5:6, :] = b_row
    counted(send_sem.at[ITERS]).wait()


def split_kernel(packed, basis, coef):
    basis[...] = packed[0:4, 0:TILE]
    coef[...] = packed[4:6, 0:ITERS]


def solution(mesh):
    vmem = pl.BlockSpec(memory_space=pltpu.VMEM)
    hbm = pl.BlockSpec(memory_space=pl.ANY)

    def local(matrix, diagonal, start):
        packed = pl.pallas_call(
            kernel,
            out_shape=pltpu.VMEM((8, LANES), jnp.float32),
            in_specs=[hbm, hbm, hbm],
            out_specs=vmem,
            scratch_shapes=[
                pltpu.VMEM((ROWS, COLS), jnp.float32),
                pltpu.VMEM((2, 1, TILE), jnp.float32),
                pltpu.VMEM((ITERS + 1, 2, LANES), jnp.float32),
                pltpu.VMEM((ITERS + 1, 8 * PAIRS, LANES), jnp.float32),
                pltpu.VMEM((3, PAIRS, LANES), jnp.float32),
                pltpu.VMEM((DEVICES - 1, 2, LANES), jnp.float32),
                pltpu.SemaphoreType.DMA,
                pltpu.SemaphoreType.DMA((2,)),
                pltpu.SemaphoreType.DMA((ITERS + 1,)),
                pltpu.SemaphoreType.DMA((ITERS + 1,)),
            ],
            compiler_params=pltpu.CompilerParams(collective_id=0, has_side_effects=True),
        )(matrix, diagonal.reshape(1, TILE), start.reshape(1, TILE))
        return pl.pallas_call(
            split_kernel,
            out_shape=(
                jax.ShapeDtypeStruct((ITERS + 1, TILE), jnp.float32),
                jax.ShapeDtypeStruct((2, ITERS), jnp.float32),
            ),
            in_specs=[vmem],
            out_specs=(vmem, vmem),
        )(pltpu.with_memory_space_constraint(packed, pltpu.VMEM))

    return jax.shard_map(
        local,
        mesh=mesh,
        in_specs=(P("row", "col"), P(("row", "col")), P(("row", "col"))),
        out_specs=(P(None, ("row", "col")), P()),
        check_vma=False,
    )
```

```python
import math

import jax
import jax.numpy as jnp
from jax import lax
from jax.experimental import pallas as pl
from jax.experimental.pallas import tpu as pltpu
from jax.sharding import PartitionSpec as P

ITERS = 3
DIM = 12288
DEVICES = 128
ROWS = 192
COLS = 6144
TILE = 96
LANES = 128
PAIRS = 32
LOGICAL = pl.DeviceIdType.LOGICAL


def hops(step):
    return (0, 1, 2, 1)[step]


STEPS = sorted(
    (
        (i, j, k, m)
        for i in range(4)
        for j in range(4)
        for k in range(4)
        for m in range(2)
        if i or j or k
    ),
    key=lambda s: (-(hops(s[0]) + hops(s[1]) + hops(s[2])), s[3]),
)


def total(value):
    return jnp.sum(value, keepdims=True)


def kernel(matrix, diagonal, start, out, mat, small, frame, planes, x_rows, slots, mat_sem, small_sem, send_sem, recv_sem):
    row = lax.axis_index("row")
    col = lax.axis_index("col")
    pair = row // 2
    odd = row % 2
    here = odd * 2 + col
    slot = here * 2 * PAIRS + pair * 2
    z, y, x = row // 16, (row // 4) % 4, row % 4
    z_part = [((z + i) % 4) * 32 for i in range(4)]
    y_part = [((y + i) % 4) * 8 for i in range(4)]
    x_part = [((x + i) % 4) * 2 for i in range(4)]
    peers = [z_part[i] + y_part[j] + x_part[k] + m for i, j, k, m in STEPS]
    peers.append(row * 2 + 1 - col)

    barrier = pltpu.get_barrier_semaphore()
    for peer in peers:
        pl.semaphore_signal(barrier, inc=1, device_id=peer, device_id_type=LOGICAL)
    load_start = pltpu.make_async_copy(start, small.at[0], small_sem.at[0])
    load_diag = pltpu.make_async_copy(diagonal, small.at[1], small_sem.at[1])
    load = pltpu.make_async_copy(matrix, mat, mat_sem)
    load_start.start()
    load_diag.start()
    load.start()

    lane = lax.broadcasted_iota(jnp.int32, (1, LANES), 1)

    def framed(part):
        wide = jnp.concatenate([part, jnp.zeros((1, LANES - TILE), jnp.float32)], axis=1)
        out = []
        for o in range(2):
            for c in range(2):
                offset = 64 * o + TILE * c
                shift = offset % LANES
                moved = pltpu.roll(wide, shift, 1) if shift else wide
                first, second = jnp.where(lane >= shift, moved, 0.0), jnp.where(lane < shift, moved, 0.0)
                zero = jnp.zeros_like(moved)
                out.append((zero, first) if offset >= LANES else (first, second))
        rows = []
        for h in range(2):
            pick = out[0][h]
            for n in range(1, 4):
                pick = jnp.where(here == n, out[n][h], pick)
            rows.append(pick)
        return rows

    def send(k, value):
        for h in range(2):
            frame[k, h : h + 1, :] = value[h]
        for peer in peers:
            pltpu.make_async_remote_copy(
                src_ref=frame.at[k],
                dst_ref=planes.at[k, pl.ds(slot, 2), :],
                send_sem=send_sem.at[k],
                recv_sem=recv_sem.at[k],
                device_id=peer,
                device_id_type=LOGICAL,
            ).start()
        for h in range(2):
            planes[k, pl.ds(slot + h, 1), :] = value[h]

    def counted(sem):
        done = slots.at[:]
        return pltpu.make_async_copy(done, done, sem)

    def receive(k):
        counted(recv_sem.at[k]).wait()
        side = [
            [planes[k, pl.ds(2 * PAIRS * n + h, PAIRS, stride=2), :] for h in range(2)] for n in range(4)
        ]
        part = [side[0][h] + side[1][h] for h in range(2)]
        rest = [side[2][h] + side[3][h] for h in range(2)]
        rows = [part[0], part[1] + rest[0], rest[1]]
        for j in range(3):
            x_rows[j] = rows[j]
        return jnp.concatenate(rows, axis=0)

    def own_rows():
        return [x_rows[odd + h, pl.ds(pair, 1), :] for h in range(2)]

    def multiply(diag):
        own = own_rows()
        acc = [None] * (ROWS // 8)
        for groups in (range(16), range(16, 24)):
            for n in range(COLS // LANES):
                value = x_rows[n % 3, pl.ds(col * (PAIRS // 2) + n // 3, 1), :]
                wide = jnp.broadcast_to(value, (8, LANES))
                for g in groups:
                    term = mat[8 * g : 8 * g + 8, n * LANES : (n + 1) * LANES] * wide
                    acc[g] = term if n == 0 else acc[g] + term
        zero = jnp.zeros((8, LANES), jnp.float32)
        is_odd = odd == 1
        padded = [
            jnp.where(is_odd, acc[t - 8] if t >= 8 else zero, acc[t] if t < 24 else zero) for t in range(32)
        ]
        rows = []
        for h in range(2):
            block = jnp.concatenate(padded[16 * h : 16 * h + 16], axis=0)
            rows.append(jnp.sum(block.T, axis=0, keepdims=True) + diag[h] * own[h])
        return rows

    def unframed(first, second):
        pick = None
        for o in range(2):
            for c in range(2):
                offset = 64 * o + TILE * c
                shift = offset % LANES
                if offset >= LANES:
                    moved = pltpu.roll(second, LANES - shift, 1)
                elif shift:
                    moved = pltpu.roll(jnp.where(lane >= shift, first, second), LANES - shift, 1)
                else:
                    moved = first
                pick = moved if pick is None else jnp.where(here == 2 * o + c, moved, pick)
        return pick

    load_start.wait()
    first = framed(small[0])
    load_diag.wait()
    diag = framed(small[1])
    pl.semaphore_wait(barrier, DEVICES - 1)
    send(0, first)
    load.wait()

    scale = jnp.float32(math.sqrt(DIM))
    known, images, slices = [], [], []
    for k in range(ITERS + 1):
        vector = receive(k)
        own = unframed(*own_rows())
        if k < ITERS:
            image = multiply(diag)
        dots = [total(q * vector) for q in known]
        for h, q, s in zip(dots, known, slices):
            vector = vector - h * q
            own = own - h * s
        norm = jnp.sqrt(total(vector * vector))
        if k < ITERS:
            for h, f in zip(dots, images):
                image = [a - h * b for a, b in zip(image, f)]
            image = [a / norm for a in image]
            send(k + 1, image)
            counted(send_sem.at[k]).wait()
            images.append(image)
            known.append(vector / norm)
        own = own / norm
        slices.append(own)
        out[k : k + 1, :] = own * scale
        if k:
            column = lane == k - 1
            a_row = jnp.where(column, dots[-1], a_row if k > 1 else 0.0)
            b_row = jnp.where(column, norm, b_row if k > 1 else 0.0)
    out[4:5, :] = a_row
    out[5:6, :] = b_row
    counted(send_sem.at[ITERS]).wait()


def split_kernel(packed, basis, coef):
    basis[...] = packed[0:4, 0:TILE]
    coef[...] = packed[4:6, 0:ITERS]


def solution(mesh):
    vmem = pl.BlockSpec(memory_space=pltpu.VMEM)
    hbm = pl.BlockSpec(memory_space=pl.ANY)

    def local(matrix, diagonal, start):
        packed = pl.pallas_call(
            kernel,
            out_shape=pltpu.VMEM((8, LANES), jnp.float32),
            in_specs=[hbm, hbm, hbm],
            out_specs=vmem,
            scratch_shapes=[
                pltpu.VMEM((ROWS, COLS), jnp.float32),
                pltpu.VMEM((2, 1, TILE), jnp.float32),
                pltpu.VMEM((ITERS + 1, 2, LANES), jnp.float32),
                pltpu.VMEM((ITERS + 1, 8 * PAIRS, LANES), jnp.float32),
                pltpu.VMEM((3, PAIRS, LANES), jnp.float32),
                pltpu.VMEM((DEVICES - 1, 2, LANES), jnp.float32),
                pltpu.SemaphoreType.DMA,
                pltpu.SemaphoreType.DMA((2,)),
                pltpu.SemaphoreType.DMA((ITERS + 1,)),
                pltpu.SemaphoreType.DMA((ITERS + 1,)),
            ],
            compiler_params=pltpu.CompilerParams(collective_id=0, has_side_effects=True),
        )(matrix, diagonal.reshape(1, TILE), start.reshape(1, TILE))
        return pl.pallas_call(
            split_kernel,
            out_shape=(
                jax.ShapeDtypeStruct((ITERS + 1, TILE), jnp.float32),
                jax.ShapeDtypeStruct((2, ITERS), jnp.float32),
            ),
            in_specs=[vmem],
            out_specs=(vmem, vmem),
        )(pltpu.with_memory_space_constraint(packed, pltpu.VMEM))

    return jax.shard_map(
        local,
        mesh=mesh,
        in_specs=(P("row", "col"), P(("row", "col")), P(("row", "col"))),
        out_specs=(P(None, ("row", "col")), P()),
        check_vma=False,
    )
```
